32 devices in a mesh: rows: 4 (over x, core), batch: 8 (over z, y).
Axes of the slice: x: 2, y: 2, z: 4, core: 2. Of those that a mesh axis runs over, the one named last changes fastest.
Arguments:
- features: bfloat16 [96, 8, 32, 512], P('batch', 'rows'), may hold values from -12 to 12
- norm_gain: float32 [512], replicated, may hold values from 0.25 to 1.75
- norm_bias: float32 [512], replicated, may hold values from -2.5 to 2.5
- conv_weight: bfloat16 [4, 4608], replicated, may hold values from -0.09375 to 0.09375
- embed_weight: float32 [16, 1024], replicated, may hold values from -1.5 to 1.5
- embed_bias: float32 [1024], replicated, may hold values from -2.5 to 2.5
- proj_in: bfloat16 [1024, 2048], P('rows'), may hold values from -0.1875 to 0.1875
- proj_in_bias: float32 [2048], replicated, may hold values from -2.5 to 2.5
- proj_out: bfloat16 [2048, 768], P('rows'), may hold values from -0.125 to 0.125
- proj_out_bias: float32 [768], replicated, may hold values from -2.5 to 2.5
- targets: bfloat16 [96, 4, 16, 768], P('batch', 'rows'), may hold values from -6 to 6
Outputs:
- grad_features: bfloat16 [96, 8, 32, 512], P('batch', 'rows')
- grad_conv: float32 [4, 4608], replicated
- grad_gain: float32 [512], replicated
- grad_bias: float32 [512], replicated
- grad_embed: float32 [16, 1024], replicated
The draws below stay inside these ranges and needn't reach their ends.
All inputs are finite; a program needn't handle non-finite values.
Results may differ from the reference program's by a relative error of at most 0.012.
Values may be sent and summed in bfloat16 or wider, within the bound.
A program may use at most 128 MiB of HBM per device.

```python
import jax
import jax.numpy as jnp
from jax import lax

CHANNELS = 512
GROUPS = 32
LATENT = 4
PATCH = 2
WIDTH = 1024
PROJ = 2048
ALIGN = 768
COLS = 32
IMAGES = 96
HEIGHT = 8
TOK_ROWS = 4
TOK_COLS = 16


def draw_features(key, part):
    key_base, key_chan = jax.random.split(key, 2)
    positions = jnp.arange(HEIGHT, dtype=jnp.float32)
    ramp = 1.0 + 2.0 * positions / max(HEIGHT - 1, 1)
    channel_scale = jnp.exp(jax.random.uniform(key_chan, (IMAGES, 1, 1, CHANNELS), minval=-0.7, maxval=0.7))
    base = jax.random.normal(key_base, (IMAGES, HEIGHT, COLS, CHANNELS))
    values = base * ramp[None, :, None, None] * channel_scale
    return jnp.clip(values, -12.0, 12.0).astype(jnp.bfloat16)


def block_levels(rng, shape, cuts, least, largest):
    def one(dim, shards_of):
        heights = jax.random.uniform(jax.random.fold_in(jax.random.fold_in(rng, 6), dim), (shards_of,), jnp.float32, least / len(cuts), largest / len(cuts))
        return jnp.repeat(jnp.exp(heights), shape[dim] // shards_of).reshape((-1,) + (1,) * (len(shape) - dim - 1))

    level = one(*cuts[0])
    for cut in cuts[1:]:
        level = level * one(*cut)
    return level


def noise(rng, dims, scale, most, cuts=(), kind=jnp.bfloat16):
    loudness = block_levels(rng, dims, cuts, -0.22, 0.18) if cuts else 1.0
    values = jax.random.normal(rng, dims, jnp.float32) * scale * loudness
    return jnp.minimum(jnp.maximum(values, -most), most).astype(kind)


def setup_inputs(seed: int = 0) -> dict:
    key_list = jax.random.split(jax.random.key(seed), 12)
    features = draw_features(jax.random.fold_in(key_list[11], 71), 0)
    norm_gain = jnp.clip(1.0 + 0.15 * jax.random.normal(key_list[1], (CHANNELS,), jnp.float32), 0.25, 1.75)
    norm_bias = noise(key_list[2], (CHANNELS,), 0.4, 2.5, (), jnp.float32)
    conv_weight = noise(key_list[3], (LATENT, 9 * CHANNELS), (9 * CHANNELS) ** -0.5, 0.09375)
    embed_weight = noise(key_list[4], (PATCH * PATCH * LATENT, WIDTH), (PATCH * PATCH * LATENT) ** -0.5, 1.5, (), jnp.float32)
    embed_bias = noise(key_list[5], (WIDTH,), 0.4, 2.5, (), jnp.float32)
    proj_in = noise(key_list[6], (WIDTH, PROJ), WIDTH ** -0.5, 0.1875, ((0, 4),))
    proj_in_bias = noise(key_list[7], (PROJ,), 0.4, 2.5, (), jnp.float32)
    proj_out = noise(key_list[8], (PROJ, ALIGN), PROJ ** -0.5, 0.125, ((0, 4),))
    proj_out_bias = noise(key_list[9], (ALIGN,), 0.4, 2.5, (), jnp.float32)
    targets = noise(key_list[10], (IMAGES, TOK_ROWS, TOK_COLS, ALIGN), 1.0, 6.0, ((0, 8), (1, 4)))
    return {"features": features, "norm_gain": norm_gain, "norm_bias": norm_bias, "conv_weight": conv_weight, "embed_weight": embed_weight, "embed_bias": embed_bias, "proj_in": proj_in, "proj_in_bias": proj_in_bias, "proj_out": proj_out, "proj_out_bias": proj_out_bias, "targets": targets}


EPS_NORM = 1e-06
EPS_UNIT = 1e-06

def swish_slope(values):
    sig = jax.nn.sigmoid(values)
    return sig * (1.0 + values * (1.0 - sig))

def one_image(feature_map, target_map, norm_gain, norm_bias, conv_weight, embed_weight, embed_bias, proj_in, proj_in_bias, proj_out, proj_out_bias):
    height, across, channels = feature_map.shape
    per_group = channels // GROUPS
    cell_count = height * across
    values = feature_map.astype(jnp.float32)
    grouped = values.reshape(cell_count, GROUPS, per_group)
    group_mean = lax.optimization_barrier(jnp.mean(grouped, axis=(0, 2), keepdims=True))
    centred = grouped - group_mean
    variance = lax.optimization_barrier(jnp.mean(centred * centred, axis=(0, 2), keepdims=True))
    inverse = lax.rsqrt(variance + EPS_NORM)
    normed = (centred * inverse).reshape(height, across, channels)
    shifted = normed * norm_gain + norm_bias
    active = (shifted * jax.nn.sigmoid(shifted)).astype(jnp.bfloat16)
    padded = jnp.pad(active, ((1, 1), (1, 1), (0, 0)))
    latent = jnp.zeros((cell_count, LATENT), jnp.float32)
    windows = []
    for position in range(9):
        row_off, col_off = (position // 3, position % 3)
        window = padded[row_off:row_off + height, col_off:col_off + across, :].reshape(cell_count, channels)
        windows.append(window)
        kernel = conv_weight[:, position * channels:(position + 1) * channels]
        latent = latent + lax.dot_general(window, kernel, (((1,), (1,)), ((), ())), preferred_element_type=jnp.float32)
    tok_rows = height // PATCH
    tok_cols = across // PATCH
    patches = latent.reshape(tok_rows, PATCH, tok_cols, PATCH, LATENT).transpose(0, 2, 1, 3, 4).reshape(tok_rows * tok_cols, PATCH * PATCH * LATENT)
    embedded = (jnp.dot(patches, embed_weight, precision=lax.Precision.HIGHEST) + embed_bias).astype(jnp.bfloat16)
    hidden_pre = jnp.dot(embedded, proj_in, preferred_element_type=jnp.float32) + proj_in_bias
    hidden_act = (hidden_pre * jax.nn.sigmoid(hidden_pre)).astype(jnp.bfloat16)
    projected = jnp.dot(hidden_act, proj_out, preferred_element_type=jnp.float32) + proj_out_bias
    target = target_map.reshape(tok_rows * tok_cols, -1).astype(jnp.float32)
    unit_target = target * lax.rsqrt(lax.optimization_barrier(jnp.sum(target * target, axis=1, keepdims=True)) + EPS_UNIT)
    inv_len = lax.rsqrt(lax.optimization_barrier(jnp.sum(projected * projected, axis=1, keepdims=True)) + EPS_UNIT)
    unit_proj = projected * inv_len
    cosine = lax.optimization_barrier(jnp.sum(unit_proj * unit_target, axis=1, keepdims=True))
    grad_out = (-inv_len * (unit_target - cosine * unit_proj)).astype(jnp.bfloat16)
    back_hidden = lax.dot_general(grad_out, proj_out, (((1,), (1,)), ((), ())), preferred_element_type=jnp.float32)
    grad_hidden = (back_hidden * swish_slope(hidden_pre)).astype(jnp.bfloat16)
    grad_embedded = lax.dot_general(grad_hidden, proj_in, (((1,), (1,)), ((), ())), preferred_element_type=jnp.float32)
    embed_part = lax.dot_general(patches, grad_embedded, (((0,), (0,)), ((), ())), precision=lax.Precision.HIGHEST)
    grad_patch = lax.dot_general(grad_embedded, embed_weight, (((1,), (1,)), ((), ())), precision=lax.Precision.HIGHEST)
    grad_latent = grad_patch.reshape(tok_rows, tok_cols, PATCH, PATCH, LATENT).transpose(0, 2, 1, 3, 4).reshape(height, across, LATENT).astype(jnp.bfloat16)
    grad_flat = grad_latent.reshape(cell_count, LATENT)
    grad_pad = jnp.pad(grad_latent, ((1, 1), (1, 1), (0, 0)))
    grad_active = jnp.zeros((cell_count, channels), jnp.float32)
    conv_parts = []
    for position in range(9):
        row_off, col_off = (position // 3, position % 3)
        conv_parts.append(lax.dot_general(grad_flat, windows[position], (((0,), (0,)), ((), ())), preferred_element_type=jnp.float32))
        back = grad_pad[2 - row_off:2 - row_off + height, 2 - col_off:2 - col_off + across, :].reshape(cell_count, LATENT)
        kernel = conv_weight[:, position * channels:(position + 1) * channels]
        grad_active = grad_active + jnp.dot(back, kernel, preferred_element_type=jnp.float32)
    conv_part = jnp.concatenate(conv_parts, axis=1)
    flat_shift = shifted.reshape(cell_count, channels)
    flat_normed = normed.reshape(cell_count, channels)
    grad_shift = grad_active * swish_slope(flat_shift)
    gain_part = lax.optimization_barrier(jnp.sum(grad_shift * flat_normed, axis=0))
    bias_part = lax.optimization_barrier(jnp.sum(grad_shift, axis=0))
    grad_norm = (grad_shift * norm_gain).reshape(cell_count, GROUPS, per_group)
    normed_groups = flat_normed.reshape(cell_count, GROUPS, per_group)
    first = lax.optimization_barrier(jnp.mean(grad_norm, axis=(0, 2), keepdims=True))
    second = lax.optimization_barrier(jnp.mean(grad_norm * normed_groups, axis=(0, 2), keepdims=True))
    grad_values = inverse * (grad_norm - first - normed_groups * second)
    grad_map = grad_values.reshape(height, across, channels).astype(jnp.bfloat16)
    return (grad_map, conv_part, gain_part, bias_part, embed_part)

def reference(features, norm_gain, norm_bias, conv_weight, embed_weight, embed_bias, proj_in, proj_in_bias, proj_out, proj_out_bias, targets):

    def step(pair):
        return one_image(pair[0], pair[1], norm_gain, norm_bias, conv_weight, embed_weight, embed_bias, proj_in, proj_in_bias, proj_out, proj_out_bias)
    grad_features, conv_parts, gain_parts, bias_parts, embed_parts = lax.map(step, (features, targets))
    return (grad_features, lax.optimization_barrier(jnp.sum(conv_parts, axis=0)), lax.optimization_barrier(jnp.sum(gain_parts, axis=0)), lax.optimization_barrier(jnp.sum(bias_parts, axis=0)), lax.optimization_barrier(jnp.sum(embed_parts, axis=0)))
```

```python
import functools

import jax
import jax.numpy as jnp
from jax import lax
from jax.experimental import pallas as pl
from jax.experimental.pallas import tpu as pltpu
from jax.sharding import PartitionSpec as P

GROUPS = 32
LATENT = 4
PATCH = 2
EPS_NORM = 1e-06
EPS_UNIT = 1e-06
F32 = jnp.float32
BF16 = jnp.bfloat16
NT = (((1,), (1,)), ((), ()))
TN = (((0,), (0,)), ((), ()))


def dot(a, b, dims=(((1,), (0,)), ((), ()))):
    return lax.dot_general(a, b, dims, preferred_element_type=F32)


def split(x, parts):
    out = []
    for _ in range(parts):
        part = x.astype(BF16).astype(F32)
        out.append(part)
        x = x - part
    return out


def exact_dot(x, exact, parts, dims=(((1,), (0,)), ((), ()))):
    rows = x.shape[0]
    full = dot(jnp.concatenate(split(x, parts), axis=0).astype(BF16), exact, dims)
    return sum(full[i * rows : (i + 1) * rows] for i in range(parts))


def kernel(
    images, height, across, n, nb, sliced,
    feat_h, gain_h, bias_h, conv_h, embw_h, embb_h, win_h, winb_h, wout_h, woutb_h, targ_h,
    out, conv_o, gain_o, bias_o, emb_o,
    feat, gain, bias, cw, we, web, win, winb, woutb, targ,
    st, sg, sg_in, nrm, slope, act, gs_ref, halo, halo_in, ghalo, ghalo_in,
    vpart, v1_in, vhalf, vs16, v2_in, vfull, vcat, pout, hact, hslope, gh_ref,
    a_ref, a16, a_in, fs, fg, fg_in, stat,
    pack, pack_in, piece, piece_in, emb, emb_in, whole, whole_emb,
    l_sem, s_send, s_recv, v_send, v_recv, x_send, x_recv,
    h_send, h_recv, g_send, g_recv, a_send, a_recv, f_send, f_recv,
    p_send, p_recv, q_send, q_recv, e_send, e_recv, w_send, w_recv, y_send, y_recv,
):
    me = lax.axis_index("rows")
    group = lax.axis_index("batch")
    cells, channels = feat.shape
    area = height * across
    per_group = channels // GROUPS
    members = n * area * per_group
    hidden = win.shape[1]
    part = win.shape[0]
    share = wout_h.shape[0]
    tokens = targ.shape[0]
    tok_cols = across // PATCH
    prev, following = lax.rem(me + n - 1, n), lax.rem(me + 1, n)
    odd = lax.rem(me, 2)
    sibling = me + 1 - 2 * odd
    sent = []

    def to(src, dst, ss, rs, where):
        copy = pltpu.make_async_remote_copy(
            src_ref=src, dst_ref=dst, send_sem=ss, recv_sem=rs,
            device_id=where, device_id_type=pl.DeviceIdType.MESH,
        )
        copy.start()
        sent.append(copy)
        return copy

    def send(src, dst, ss, rs, peer):
        return to(src, dst, ss, rs, {"rows": peer})

    def spread(src, dst, ss, rs):
        return [
            send(src, dst.at[k - 1], ss.at[k - 1], rs.at[k - 1], lax.rem(me + k, n))
            for k in range(1, n)
        ]

    def across_batch(src, dst, ss, rs):
        return [
            to(src, dst.at[k - 1], ss.at[k - 1], rs.at[k - 1], {"batch": lax.rem(group + k, nb)})
            for k in range(1, nb)
        ]

    def arrive(copies):
        for copy in copies:
            copy.wait_recv()

    barrier = pltpu.get_barrier_semaphore()
    for k in range(1, n):
        pl.semaphore_signal(
            barrier, inc=1, device_id={"rows": lax.rem(me + k, n)},
            device_id_type=pl.DeviceIdType.MESH,
        )
    for k in range(1, nb):
        pl.semaphore_signal(
            barrier, inc=1, device_id={"batch": lax.rem(group + k, nb)},
            device_id_type=pl.DeviceIdType.MESH,
        )

    def slab(owner):
        return pl.ds(pl.multiple_of(owner * share, share), share)

    if sliced:
        cols = pl.ds(pl.multiple_of(me * part, part), part)
        embw_v, embb_v = embw_h.at[:, cols], embb_h.at[:, cols]
    else:
        embw_v, embb_v = embw_h, embb_h
    loads = [
        pltpu.make_async_copy(src, dst, l_sem.at[i])
        for i, (src, dst) in enumerate([
            (feat_h, feat), (embw_v, we), (embb_v, web), (win_h, win),
            (wout_h, pout.at[slab(me), :]), (conv_h, cw), (gain_h, gain), (bias_h, bias),
            (winb_h, winb), (woutb_h, woutb), (targ_h, targ),
        ])
    ]
    for load in loads:
        load.start()

    st[...] = jnp.zeros_like(st)
    fs[...] = jnp.zeros_like(fs)
    pool = jnp.where(
        lax.broadcasted_iota(jnp.int32, (channels, 128), 0) // per_group
        == lax.broadcasted_iota(jnp.int32, (channels, 128), 1),
        1.0, 0.0,
    ).astype(BF16)
    loads[0].wait()

    def stats(b, carry):
        x = feat[pl.ds(pl.multiple_of(b * area, area), area), :].astype(F32)
        total = jnp.sum(x, axis=0, keepdims=True)
        centred = x - total / area
        st[0, pl.ds(b, 1), :] = total
        st[1, pl.ds(b, 1), :] = jnp.sum(centred * centred, axis=0, keepdims=True)
        return carry

    lax.fori_loop(0, images, stats, 0)
    count = area * per_group
    group_total = exact_dot(st[0], pool, 3)
    local_mean = exact_dot(group_total / count, pool, 3, NT)
    sg[0] = group_total
    sg[1] = exact_dot(st[1] + area * jnp.square(st[0] / area - local_mean), pool, 3)

    for load in loads[1:4]:
        load.wait()
    first_row = lax.broadcasted_iota(jnp.int32, (8, part), 0) == 0
    wcat = jnp.concatenate([we[...], jnp.where(first_row, web[...], 0.0)], axis=0)
    vpart[...] = exact_dot(wcat, win[...], 2)
    for load in loads[4:]:
        load.wait()
    pl.semaphore_wait(barrier, n + nb - 2)

    half = hidden // 2
    mine = pl.ds(pl.multiple_of(odd * half, half), half)
    theirs = pl.ds(pl.multiple_of((1 - odd) * half, half), half)
    v1 = send(vpart.at[:, theirs], v1_in, v_send.at[0], v_recv.at[0], sibling)
    stat_copies = spread(sg, sg_in, s_send, s_recv)

    quarter = share // 4
    fine = quarter // 4 if (quarter // 4) % 16 == 0 else quarter // 2
    parts = {
        "a": (0, quarter // 2), "b1": (quarter // 2, fine), "b2": (quarter // 2 + fine, quarter // 2 - fine),
        "d": (quarter // 2, quarter // 2), "e1": (0, fine), "e2": (fine, quarter // 2 - fine),
    }
    q0 = lax.rem(group, 4)
    q1 = q0 + 1 - 2 * lax.rem(q0, 2)
    q2 = lax.rem(q0 + 2, 4)
    q3 = lax.rem(q1 + 2, 4)
    y_peer = {"batch": group + 1 - 2 * lax.rem(group, 2)}
    z_peer = {"batch": group - q0 + q2}
    ring = n // 2 - 1
    names = [
        ("x", "a", q0), ("x", "b1", q0), ("x", "b2", q0), ("x", "d", q3),
        ("y", "a", q1), ("y", "b1", q1), ("y", "b2", q1), ("y", "e2", q3),
        ("z", "a", q2), ("z", "b1", q2), ("z", "b2", q2), ("z", "e1", q3),
    ]
    names = [item for item in names if parts[item[1]][1]]
    slot = {(link, name): i for i, (link, name, _) in enumerate(names)}
    arriving = {}
    relays = []

    def block(owner, q, name):
        start, size = parts[name]
        unit = min(size, fine)
        return pout.at[pl.ds(pl.multiple_of(owner * share + q * quarter + start, unit), size), :]

    def owner_of(k):
        return lax.rem(me + n - 2 * k, n)

    def push(link, name, k, owner, q, where):
        if not parts[name][1]:
            return
        i = (k - 1) * 2 * len(names) + slot[link, name]
        ref = block(owner, q, name)
        arriving[link, name, k] = to(ref, ref, x_send.at[i], x_recv.at[i], where)

    def over_x(name):
        for k in range(1, ring + 1):
            push("x", name, k, me, q3 if name == "d" else q0, {"rows": lax.rem(me + 2 * k, n)})

    def relay(link, name, onward=()):
        q = {item[:2]: item[2] for item in names}
        for k in range(1, ring + 1):
            if (link, name, k) not in arriving:
                continue
            arriving[link, name, k].wait_recv()
            for next_link, next_name in onward:
                push(
                    next_link, next_name, k, owner_of(k), q[link, name],
                    y_peer if next_link == "y" else z_peer,
                )
            i = ((k - 1) * 2 + 1) * len(names) + slot[link, name]
            ref = block(owner_of(k), q[link, name], name)
            relays.append(to(ref, ref, x_send.at[i], x_recv.at[i], {"rows": sibling}))

    over_x("a")
    last = 2 * ring * len(names)
    own = pout.at[slab(me), :]
    beside = send(own, own, x_send.at[last], x_recv.at[last], sibling)

    v1.wait_recv()
    v_half = vpart[:, mine] + v1_in[...]
    vhalf[...] = v_half
    vs16[...] = v_half.astype(BF16)
    v2 = [
        send(vs16, v2_in.at[k - 1], v_send.at[k], v_recv.at[k], lax.rem(me + 2 * k, n))
        for k in range(1, ring + 1)
    ]
    over_x("b1")

    weights = cw[...].astype(F32)
    weights = jnp.concatenate([weights, weights], axis=0)
    taps = jnp.concatenate(
        [weights[:, t * channels : (t + 1) * channels] for t in range(9)], axis=0
    ).astype(BF16)

    arrive(stat_copies)
    sums = [sg[0]] + [sg_in[k, 0] for k in range(n - 1)]
    squares = [sg[1]] + [sg_in[k, 1] for k in range(n - 1)]
    mean = sum(sums) / members
    variance = sum(
        sq + count * jnp.square(total / count - mean) for total, sq in zip(sums, squares)
    ) / members
    rows = mean.shape[0]
    both_stats = exact_dot(
        jnp.concatenate([mean, lax.rsqrt(variance + EPS_NORM)], axis=0), pool, 3, NT
    )
    stat[0] = both_stats[0:rows]
    stat[1] = both_stats[rows:]

    def forward(b, carry):
        where = pl.ds(pl.multiple_of(b * area, area), area)
        x = feat[where, :].astype(F32)
        normed = (x - stat[0, pl.ds(b, 1), :]) * stat[1, pl.ds(b, 1), :]
        shifted = normed * gain[...] + bias[...]
        sig = jax.nn.sigmoid(shifted)
        nrm[where, :] = normed
        act[where, :] = (shifted * sig).astype(BF16)
        slope[where, :] = sig * (1.0 + shifted * (1.0 - sig))
        return carry

    lax.fori_loop(0, images, forward, 0)

    lane = lax.broadcasted_iota(jnp.int32, (8, cells), 1)
    col = lax.rem(lane, across)
    row = lax.rem(lane // across, height)

    def ahead(x, count):
        return pltpu.roll(x, (-count) % cells, 1) if count % cells else x

    def beside_col(x, off):
        if off == 0:
            return x
        ok = (col + off >= 0) & (col + off < across)
        return jnp.where(ok, ahead(x, off), 0.0)

    def above(x, arrived):
        edge = jnp.where(me > 0, ahead(arrived, (height - 1) * across), 0.0)
        return jnp.where(row == 0, edge, ahead(x, -across))

    def below(x, arrived):
        edge = jnp.where(me < n - 1, ahead(arrived, -(height - 1) * across), 0.0)
        return jnp.where(row == height - 1, edge, ahead(x, across))

    terms = dot(taps, act[...], NT)
    rows3 = []
    for dy in range(3):
        rows3.append(
            sum(
                beside_col(terms[(3 * dy + dx) * 8 : (3 * dy + dx + 1) * 8], dx - 1)
                for dx in range(3)
            )
        )
    halo[0] = rows3[0]
    halo[1] = rows3[2]
    halo_copies = [
        send(halo.at[0], halo_in.at[0], h_send.at[0], h_recv.at[0], following),
        send(halo.at[1], halo_in.at[1], h_send.at[1], h_recv.at[1], prev),
    ]
    over_x("b2")
    over_x("d")
    relay("x", "a", (("y", "a"), ("z", "a")))
    cell = lax.broadcasted_iota(jnp.int32, (cells, tokens), 0)
    tok = lax.broadcasted_iota(jnp.int32, (cells, tokens), 1)
    per_image = (height // PATCH) * tok_cols
    corner = (
        (tok // per_image) * area
        + (lax.rem(tok, per_image) // tok_cols) * (PATCH * across)
        + lax.rem(tok, tok_cols) * PATCH
    )
    away = cell - corner
    pick = [
        jnp.where(away == u * across + v, 1.0, 0.0).astype(BF16)
        for u in range(PATCH) for v in range(PATCH)
    ]
    arrive(v2)
    vfull[:, mine] = vhalf[...] + sum(v2_in[k].astype(F32) for k in range(ring))
    v3 = send(vfull.at[:, mine], vfull.at[:, mine], v_send.at[ring + 1], v_recv.at[ring + 1], sibling)
    arrive(halo_copies)
    relay("x", "b1", (("y", "b1"), ("z", "b1")))
    inner = PATCH * PATCH * LATENT
    latent = rows3[1] + above(rows3[0], halo_in[0]) + below(rows3[2], halo_in[1])
    first_half = lax.broadcasted_iota(jnp.int32, (8, tokens), 0) < LATENT
    blocks = []
    for u in range(PATCH):
        pair = [exact_dot(latent, pick[u * PATCH + v], 3) for v in range(PATCH)]
        blocks.append(jnp.where(first_half, pair[0], pair[1]))
    patches = jnp.concatenate(blocks, axis=0)
    p_hi, p_lo = split(patches, 2)
    pcat = jnp.concatenate([p_hi, p_lo, p_hi], axis=0).astype(BF16)
    v3.wait_recv()
    v_hi, v_lo = split(vfull[0:inner, :], 2)
    vcat[...] = jnp.concatenate([v_hi, v_hi, v_lo], axis=0).astype(BF16)
    pre_bias = vfull[inner : inner + 1, :] + winb[...]

    step = hidden // 4
    for c in range(4):
        where = slice(c * step, (c + 1) * step)
        pre = dot(pcat, vcat[:, where], TN) + pre_bias[:, where]
        sig = jax.nn.sigmoid(pre)
        hact[:, where] = (pre * sig).astype(BF16)
        hslope[:, where] = sig * (1.0 + pre * (1.0 - sig))
    relay("x", "b2", (("y", "b2"), ("z", "b2")))
    relay("y", "a", (("z", "e1"),))
    relay("z", "a", (("y", "e2"),))
    target = targ[...].astype(F32)
    unit_target = target * lax.rsqrt(jnp.sum(target * target, axis=1, keepdims=True) + EPS_UNIT)
    beside.wait_recv()
    pair_of = me // 2

    def pair_dot(j):
        base = lax.rem(pair_of + j, n // 2) * (2 * share)
        where = pl.ds(pl.multiple_of(base, 2 * share), 2 * share)
        return dot(hact[:, where], pout[where, :])

    bias_out = jnp.concatenate([woutb[i : i + 1, :] for i in range(woutb.shape[0])], axis=1)
    projected = pair_dot(0) + bias_out
    relay("y", "b1")
    relay("z", "b1")
    relay("x", "d")
    relay("y", "b2")
    relay("z", "b2")
    relay("z", "e1")
    relay("y", "e2")
    arrive(relays)
    for j in range(1, n // 2):
        projected = projected + pair_dot(j)
    inv_len = lax.rsqrt(jnp.sum(projected * projected, axis=1, keepdims=True) + EPS_UNIT)
    unit_proj = projected * inv_len
    cosine = jnp.sum(unit_proj * unit_target, axis=1, keepdims=True)
    grad_out = (-inv_len * (unit_target - cosine * unit_proj)).astype(BF16)
    for c in range(4):
        where = slice(c * step, (c + 1) * step)
        back = dot(grad_out, pout[where, :], NT)
        gh_ref[:, where] = (back * hslope[:, where]).astype(BF16)
    two = dot(vcat[inner:, :], gh_ref[...], NT)
    grad_patch = (two[0:inner] + two[inner:]).astype(BF16)

    grid = []
    for v in range(PATCH):
        grid.append(
            sum(
                dot(grad_patch[u * 8 : (u + 1) * 8], pick[u * PATCH + v], NT)
                for u in range(PATCH)
            )
        )
    low_rows = lax.broadcasted_iota(jnp.int32, (8, cells), 0) < LATENT
    both = jnp.where(low_rows, grid[0], grid[1])
    grad_lat = both + pltpu.roll(both, LATENT, 0)
    grad_lat = jnp.where(low_rows, grad_lat, 0.0)
    ghalo[...] = grad_lat
    ghalo_copies = [
        send(ghalo, ghalo_in.at[0], g_send.at[0], g_recv.at[0], following),
        send(ghalo, ghalo_in.at[1], g_send.at[1], g_recv.at[1], prev),
    ]
    wide = dot(pcat[0 : 2 * inner], gh_ref[...])
    a_sum = wide[0:inner] + wide[inner:]
    a_ref[...] = a_sum
    a16[...] = a_sum.astype(BF16)
    a_copies = spread(a16, a_in, a_send, a_recv)
    arrive(ghalo_copies)
    by_row = [below(grad_lat, ghalo_in[1]), grad_lat, above(grad_lat, ghalo_in[0])]
    grad_taps = jnp.concatenate(
        [beside_col(by_row[dy], 1 - dx) for dy in range(3) for dx in range(3)], axis=0
    ).astype(BF16)
    gs_ref[...] = dot(grad_taps, taps, TN)
    conv = dot(grad_taps, act[...])

    def backward(b, carry):
        where = pl.ds(pl.multiple_of(b * area, area), area)
        gs = gs_ref[where, :] * slope[where, :]
        gs_ref[where, :] = gs
        fs[0, pl.ds(b, 1), :] = jnp.sum(gs, axis=0, keepdims=True)
        fs[1, pl.ds(b, 1), :] = jnp.sum(gs * nrm[where, :], axis=0, keepdims=True)
        return carry

    lax.fori_loop(0, images, backward, 0)
    pooled = exact_dot(jnp.concatenate([fs[0] * gain[...], fs[1] * gain[...]], axis=0), pool, 3)
    fg[0] = pooled[0:rows]
    fg[1] = pooled[rows:]
    f_copies = spread(fg, fg_in, f_send, f_recv)
    gain_row = jnp.sum(fs[1], axis=0, keepdims=True)
    bias_row = jnp.sum(fs[0], axis=0, keepdims=True)
    row8 = lax.broadcasted_iota(jnp.int32, (8, channels), 0)
    per = pack.shape[1] // 8
    lanes = pack.shape[2]
    for i in range(5):
        part_i = conv[16 * i : 16 * i + 8]
        if i < 4:
            part_i = part_i + pltpu.roll(conv[16 * i + 8 : 16 * i + 16], LATENT, 0)
        else:
            part_i = jnp.where(row8 == LATENT, gain_row, part_i)
            part_i = jnp.where(row8 == LATENT + 1, bias_row, part_i)
        for c in range(channels // lanes):
            t = 5 * c + i
            pack[t // per, (t % per) * 8 : (t % per + 1) * 8, :] = (
                part_i[:, c * lanes : (c + 1) * lanes]
            )
    for t in range(5 * (channels // lanes), n * per):
        pack[t // per, (t % per) * 8 : (t % per + 1) * 8, :] = jnp.zeros((8, lanes), F32)
    p_copies = []
    for k in range(1, n):
        peer = lax.rem(me + k, n)
        p_copies.append(
            send(pack.at[peer], pack_in.at[k - 1], p_send.at[k - 1], p_recv.at[k - 1], peer)
        )
    arrive(a_copies)
    a_all = a_ref[...] + sum(a_in[k].astype(F32) for k in range(n - 1))
    emb[...] = exact_dot(a_all, win[...], 2, NT).astype(BF16)
    q_copies = across_batch(emb, emb_in, e_send, e_recv)
    arrive(p_copies)
    piece[...] = (pack[me] + sum(pack_in[k] for k in range(n - 1))).astype(BF16)
    piece_copies = across_batch(piece, piece_in, q_send, q_recv)
    arrive(f_copies)
    totals = [(fg[i] + sum(fg_in[k, i] for k in range(n - 1))) / members for i in range(2)]
    both_means = exact_dot(jnp.concatenate(totals, axis=0), pool, 3, NT)
    stat[2] = both_means[0:rows]
    stat[3] = both_means[rows:]

    def finish(b, carry):
        where = pl.ds(pl.multiple_of(b * area, area), area)
        one = pl.ds(b, 1)
        out[where, :] = (
            stat[1, one, :]
            * (gs_ref[where, :] * gain[...] - stat[2, one, :] - nrm[where, :] * stat[3, one, :])
        ).astype(BF16)
        return carry

    lax.fori_loop(0, images, finish, 0)
    arrive(q_copies)
    whole_emb[me] = ordered(emb, emb_in, group, nb)
    w_copies = []
    for k in range(1, n):
        peer = lax.rem(me + k, n)
        w_copies.append(
            send(whole_emb.at[me], whole_emb.at[me], y_send.at[k - 1], y_recv.at[k - 1], peer)
        )
    arrive(piece_copies)
    whole[me] = ordered(piece, piece_in, group, nb)
    for k in range(1, n):
        peer = lax.rem(me + k, n)
        w_copies.append(send(whole.at[me], whole.at[me], w_send.at[k - 1], w_recv.at[k - 1], peer))
    arrive(w_copies)
    for c in range(channels // lanes):
        at = slice(c * lanes, (c + 1) * lanes)
        for i in range(5):
            t = 5 * c + i
            tile = whole[t // per, (t % per) * 8 : (t % per + 1) * 8, :]
            for side in range(2):
                tap = 2 * i + side
                tile_rows = tile[side * LATENT : (side + 1) * LATENT]
                if tap < 9:
                    start = tap * channels + c * lanes
                    conv_o[:, start : start + lanes] = tile_rows
                else:
                    gain_o[:, at] = tile_rows[0:1]
                    bias_o[:, at] = tile_rows[1:2]
    for k in range(n):
        emb_o[:, k * part : (k + 1) * part] = whole_emb[k]
    for copy in sent:
        copy.wait_send()


def ordered(own, arrived, group, nb):
    total = None
    for g in range(nb):
        slot = lax.rem(group + nb - g, nb)
        value = arrived[jnp.maximum(slot - 1, 0)] if nb > 1 else own[...]
        value = jnp.where(slot == 0, own[...].astype(F32), value.astype(F32))
        total = value if total is None else total + value
    return total


def store(*refs):
    count = (len(refs) - 1) // 2
    sem = refs[-1]
    copies = [
        pltpu.make_async_copy(refs[i], refs[count + i], sem.at[i]) for i in range(count)
    ]
    for copy in copies:
        copy.start()
    for copy in copies:
        copy.wait()


def shards(
    features, norm_gain, norm_bias, conv_weight, embed_weight, embed_bias,
    proj_in, proj_in_bias, proj_out, proj_out_bias, targets,
):
    images, height, across, channels = features.shape
    n = lax.axis_size("rows")
    nb = lax.axis_size("batch")
    lanes = 128
    per = -(-(5 * (channels // lanes)) // n)
    cells = images * height * across
    align = targets.shape[-1]
    tokens = targets.shape[0] * targets.shape[1] * targets.shape[2]
    inner, width = embed_weight.shape
    part, hidden = proj_in.shape
    share = proj_out.shape[0]
    pad_images = -(-images // 8) * 8
    sliced = part % lanes == 0
    embed_bias = embed_bias[None]
    if not sliced:
        me = lax.axis_index("rows")
        embed_weight = lax.dynamic_slice_in_dim(embed_weight, me * part, part, axis=1)
        embed_bias = lax.dynamic_slice_in_dim(embed_bias, me * part, part, axis=1)
    ring = n // 2 - 1
    cols = hidden // 2
    last = max(nb - 1, 1)
    dma = pltpu.SemaphoreType.DMA
    vm = pltpu.VMEM
    results = pl.pallas_call(
        functools.partial(kernel, images, height, across, n, nb, sliced),
        out_shape=(
            vm((cells, channels), BF16),
            vm((LATENT, 9 * channels), F32),
            vm((1, channels), F32),
            vm((1, channels), F32),
            vm((inner, width), F32),
        ),
        in_specs=[pl.BlockSpec(memory_space=pltpu.HBM)] * 11,
        out_specs=[pl.BlockSpec(memory_space=vm)] * 5,
        scratch_shapes=[
            vm((cells, channels), BF16),
            vm((1, channels), F32),
            vm((1, channels), F32),
            vm((LATENT, 9 * channels), BF16),
            vm((inner, part), F32),
            vm((1, part), F32),
            vm((part, hidden), BF16),
            vm((1, hidden), F32),
            vm((align // lanes, lanes), F32),
            vm((tokens, align), BF16),
            vm((2, pad_images, channels), F32),
            vm((2, pad_images, lanes), F32),
            vm((n - 1, 2, pad_images, lanes), F32),
            vm((cells, channels), F32),
            vm((cells, channels), F32),
            vm((cells, channels), BF16),
            vm((cells, channels), F32),
            vm((2, 8, cells), F32),
            vm((2, 8, cells), F32),
            vm((8, cells), F32),
            vm((2, 8, cells), F32),
            vm((inner + 8, hidden), F32),
            vm((inner + 8, cols), F32),
            vm((inner + 8, cols), F32),
            vm((inner + 8, cols), BF16),
            vm((max(ring, 1), inner + 8, cols), BF16),
            vm((inner + 8, hidden), F32),
            vm((3 * inner, hidden), BF16),
            vm((n * share, align), BF16),
            vm((tokens, hidden), BF16),
            vm((tokens, hidden), F32),
            vm((tokens, hidden), BF16),
            vm((inner, hidden), F32),
            vm((inner, hidden), BF16),
            vm((n - 1, inner, hidden), BF16),
            vm((2, pad_images, channels), F32),
            vm((2, pad_images, lanes), F32),
            vm((n - 1, 2, pad_images, lanes), F32),
            vm((4, pad_images, channels), F32),
            vm((n, per * 8, lanes), F32),
            vm((n - 1, per * 8, lanes), F32),
            vm((per * 8, lanes), BF16),
            vm((last, per * 8, lanes), BF16),
            vm((inner, part), BF16),
            vm((last, inner, part), BF16),
            vm((n, per * 8, lanes), F32),
            vm((n, inner, part), F32),
            dma((11,)), dma((n - 1,)), dma((n - 1,)),
            dma((ring + 2,)), dma((ring + 2,)),
            dma((24 * ring + 1,)), dma((24 * ring + 1,)),
            dma((2,)), dma((2,)), dma((2,)), dma((2,)),
            dma((n - 1,)), dma((n - 1,)), dma((n - 1,)), dma((n - 1,)),
            dma((n - 1,)), dma((n - 1,)),
            dma((last,)), dma((last,)), dma((last,)), dma((last,)),
            dma((n - 1,)), dma((n - 1,)), dma((n - 1,)), dma((n - 1,)),
        ],
        compiler_params=pltpu.CompilerParams(
            collective_id=0, has_side_effects=True, vmem_limit_bytes=48 * 1024 * 1024
        ),
        name="alignment_step",
    )(
        features.reshape(cells, channels), norm_gain[None], norm_bias[None], conv_weight,
        embed_weight, embed_bias, proj_in, proj_in_bias[None], proj_out,
        proj_out_bias.reshape(align // lanes, lanes), targets.reshape(tokens, align),
    )
    grad_features, grad_conv, grad_gain, grad_bias, grad_embed = pl.pallas_call(
        store,
        out_shape=tuple(jax.ShapeDtypeStruct(x.shape, x.dtype) for x in results),
        in_specs=[pl.BlockSpec(memory_space=vm)] * 5,
        out_specs=[pl.BlockSpec(memory_space=pltpu.HBM)] * 5,
        scratch_shapes=[dma((5,))],
        compiler_params=pltpu.CompilerParams(vmem_limit_bytes=4 * 1024 * 1024),
        name="store_results",
    )(*results)
    return (
        grad_features.reshape(images, height, across, channels),
        grad_conv, grad_gain[0], grad_bias[0], grad_embed,
    )


def solution(mesh):
    in_specs = (
        P("batch", "rows", None, None), P(), P(), P(), P(), P(),
        P("rows", None), P(), P("rows", None), P(), P("batch", "rows", None, None),
    )
    out_specs = (P("batch", "rows", None, None), P(), P(), P(), P())
    return jax.shard_map(shards, mesh=mesh, in_specs=in_specs, out_specs=out_specs, check_vma=False)
```

```python
import functools

import jax
import jax.numpy as jnp
from jax import lax
from jax.experimental import pallas as pl
from jax.experimental.pallas import tpu as pltpu
from jax.sharding import PartitionSpec as P

GROUPS = 32
LATENT = 4
PATCH = 2
EPS_NORM = 1e-06
EPS_UNIT = 1e-06
F32 = jnp.float32
BF16 = jnp.bfloat16
NT = (((1,), (1,)), ((), ()))
TN = (((0,), (0,)), ((), ()))


def dot(a, b, dims=(((1,), (0,)), ((), ()))):
    return lax.dot_general(a, b, dims, preferred_element_type=F32)


def split(x, parts):
    out = []
    for _ in range(parts):
        part = x.astype(BF16).astype(F32)
        out.append(part)
        x = x - part
    return out


def exact_dot(x, exact, parts, dims=(((1,), (0,)), ((), ()))):
    rows = x.shape[0]
    full = dot(jnp.concatenate(split(x, parts), axis=0).astype(BF16), exact, dims)
    return sum(full[i * rows : (i + 1) * rows] for i in range(parts))


def kernel(
    images, height, across, n, nb, sliced,
    feat_h, gain_h, bias_h, conv_h, embw_h, embb_h, win_h, winb_h, wout_h, woutb_h, targ_h,
    out, conv_o, gain_o, bias_o, emb_o,
    feat, gain, bias, cw, we, web, win, winb, woutb, targ,
    st, sg, sg_in, nrm, slope, act, gs_ref, halo, halo_in, ghalo, ghalo_in,
    vpart, v1_in, vhalf, vs16, v2_in, vfull, vcat, pout, hact, hslope, gh_ref,
    a_ref, a16, a_in, fs, fg, fg_in, stat,
    pack, pack_in, piece, piece_in, emb, emb_in, whole, whole_emb,
    l_sem, s_send, s_recv, v_send, v_recv, x_send, x_recv,
    h_send, h_recv, g_send, g_recv, a_send, a_recv, f_send, f_recv,
    p_send, p_recv, q_send, q_recv, e_send, e_recv, w_send, w_recv, y_send, y_recv,
):
    me = lax.axis_index("rows")
    group = lax.axis_index("batch")
    cells, channels = feat.shape
    area = height * across
    per_group = channels // GROUPS
    members = n * area * per_group
    hidden = win.shape[1]
    part = win.shape[0]
    share = wout_h.shape[0]
    tokens = targ.shape[0]
    tok_cols = across // PATCH
    prev, following = lax.rem(me + n - 1, n), lax.rem(me + 1, n)
    odd = lax.rem(me, 2)
    sibling = me + 1 - 2 * odd
    sent = []

    def to(src, dst, ss, rs, where):
        copy = pltpu.make_async_remote_copy(
            src_ref=src, dst_ref=dst, send_sem=ss, recv_sem=rs,
            device_id=where, device_id_type=pl.DeviceIdType.MESH,
        )
        copy.start()
        sent.append(copy)
        return copy

    def send(src, dst, ss, rs, peer):
        return to(src, dst, ss, rs, {"rows": peer})

    def spread(src, dst, ss, rs):
        return [
            send(src, dst.at[k - 1], ss.at[k - 1], rs.at[k - 1], lax.rem(me + k, n))
            for k in range(1, n)
        ]

    def across_batch(src, dst, ss, rs):
        return [
            to(src, dst.at[k - 1], ss.at[k - 1], rs.at[k - 1], {"batch": lax.rem(group + k, nb)})
            for k in range(1, nb)
        ]

    def arrive(copies):
        for copy in copies:
            copy.wait_recv()

    barrier = pltpu.get_barrier_semaphore()
    for k in range(1, n):
        pl.semaphore_signal(
            barrier, inc=1, device_id={"rows": lax.rem(me + k, n)},
            device_id_type=pl.DeviceIdType.MESH,
        )
    for k in range(1, nb):
        pl.semaphore_signal(
            barrier, inc=1, device_id={"batch": lax.rem(group + k, nb)},
            device_id_type=pl.DeviceIdType.MESH,
        )

    def slab(owner):
        return pl.ds(pl.multiple_of(owner * share, share), share)

    if sliced:
        cols = pl.ds(pl.multiple_of(me * part, part), part)
        embw_v, embb_v = embw_h.at[:, cols], embb_h.at[:, cols]
    else:
        embw_v, embb_v = embw_h, embb_h
    loads = [
        pltpu.make_async_copy(src, dst, l_sem.at[i])
        for i, (src, dst) in enumerate([
            (feat_h, feat), (embw_v, we), (embb_v, web), (win_h, win),
            (wout_h, pout.at[slab(me), :]), (conv_h, cw), (gain_h, gain), (bias_h, bias),
            (winb_h, winb), (woutb_h, woutb), (targ_h, targ),
        ])
    ]
    for load in loads:
        load.start()

    st[...] = jnp.zeros_like(st)
    fs[...] = jnp.zeros_like(fs)
    pool = jnp.where(
        lax.broadcasted_iota(jnp.int32, (channels, 128), 0) // per_group
        == lax.broadcasted_iota(jnp.int32, (channels, 128), 1),
        1.0, 0.0,
    ).astype(BF16)
    loads[0].wait()

    def stats(b, carry):
        x = feat[pl.ds(pl.multiple_of(b * area, area), area), :].astype(F32)
        total = jnp.sum(x, axis=0, keepdims=True)
        centred = x - total / area
        st[0, pl.ds(b, 1), :] = total
        st[1, pl.ds(b, 1), :] = jnp.sum(centred * centred, axis=0, keepdims=True)
        return carry

    lax.fori_loop(0, images, stats, 0)
    count = area * per_group
    group_total = exact_dot(st[0], pool, 3)
    local_mean = exact_dot(group_total / count, pool, 3, NT)
    sg[0] = group_total
    sg[1] = exact_dot(st[1] + area * jnp.square(st[0] / area - local_mean), pool, 3)

    for load in loads[1:4]:
        load.wait()
    first_row = lax.broadcasted_iota(jnp.int32, (8, part), 0) == 0
    wcat = jnp.concatenate([we[...], jnp.where(first_row, web[...], 0.0)], axis=0)
    vpart[...] = exact_dot(wcat, win[...], 2)
    for load in loads[4:]:
        load.wait()
    pl.semaphore_wait(barrier, n + nb - 2)

    half = hidden // 2
    mine = pl.ds(pl.multiple_of(odd * half, half), half)
    theirs = pl.ds(pl.multiple_of((1 - odd) * half, half), half)
    v1 = send(vpart.at[:, theirs], v1_in, v_send.at[0], v_recv.at[0], sibling)
    stat_copies = spread(sg, sg_in, s_send, s_recv)

    quarter = share // 4
    fine = quarter // 4 if (quarter // 4) % 16 == 0 else quarter // 2
    parts = {
        "a": (0, quarter // 2), "b1": (quarter // 2, fine), "b2": (quarter // 2 + fine, quarter // 2 - fine),
        "d": (quarter // 2, quarter // 2), "e1": (0, fine), "e2": (fine, quarter // 2 - fine),
    }
    q0 = lax.rem(group, 4)
    q1 = q0 + 1 - 2 * lax.rem(q0, 2)
    q2 = lax.rem(q0 + 2, 4)
    q3 = lax.rem(q1 + 2, 4)
    y_peer = {"batch": group + 1 - 2 * lax.rem(group, 2)}
    z_peer = {"batch": group - q0 + q2}
    ring = n // 2 - 1
    names = [
        ("x", "a", q0), ("x", "b1", q0), ("x", "b2", q0), ("x", "d", q3),
        ("y", "a", q1), ("y", "b1", q1), ("y", "b2", q1), ("y", "e2", q3),
        ("z", "a", q2), ("z", "b1", q2), ("z", "b2", q2), ("z", "e1", q3),
    ]
    names = [item for item in names if parts[item[1]][1]]
    slot = {(link, name): i for i, (link, name, _) in enumerate(names)}
    arriving = {}
    relays = []

    def block(owner, q, name):
        start, size = parts[name]
        unit = min(size, fine)
        return pout.at[pl.ds(pl.multiple_of(owner * share + q * quarter + start, unit), size), :]

    def owner_of(k):
        return lax.rem(me + n - 2 * k, n)

    def push(link, name, k, owner, q, where):
        if not parts[name][1]:
            return
        i = (k - 1) * 2 * len(names) + slot[link, name]
        ref = block(owner, q, name)
        arriving[link, name, k] = to(ref, ref, x_send.at[i], x_recv.at[i], where)

    def over_x(name):
        for k in range(1, ring + 1):
            push("x", name, k, me, q3 if name == "d" else q0, {"rows": lax.rem(me + 2 * k, n)})

    def relay(link, name, onward=()):
        q = {item[:2]: item[2] for item in names}
        for k in range(1, ring + 1):
            if (link, name, k) not in arriving:
                continue
            arriving[link, name, k].wait_recv()
            for next_link, next_name in onward:
                push(
                    next_link, next_name, k, owner_of(k), q[link, name],
                    y_peer if next_link == "y" else z_peer,
                )
            i = ((k - 1) * 2 + 1) * len(names) + slot[link, name]
            ref = block(owner_of(k), q[link, name], name)
            relays.append(to(ref, ref, x_send.at[i], x_recv.at[i], {"rows": sibling}))

    over_x("a")
    last = 2 * ring * len(names)
    own = pout.at[slab(me), :]
    beside = send(own, own, x_send.at[last], x_recv.at[last], sibling)

    v1.wait_recv()
    v_half = vpart[:, mine] + v1_in[...]
    vhalf[...] = v_half
    vs16[...] = v_half.astype(BF16)
    v2 = [
        send(vs16, v2_in.at[k - 1], v_send.at[k], v_recv.at[k], lax.rem(me + 2 * k, n))
        for k in range(1, ring + 1)
    ]
    over_x("b1")

    weights = cw[...].astype(F32)
    weights = jnp.concatenate([weights, weights], axis=0)
    taps = jnp.concatenate(
        [weights[:, t * channels : (t + 1) * channels] for t in range(9)], axis=0
    ).astype(BF16)

    arrive(stat_copies)
    sums = [sg[0]] + [sg_in[k, 0] for k in range(n - 1)]
    squares = [sg[1]] + [sg_in[k, 1] for k in range(n - 1)]
    mean = sum(sums) / members
    variance = sum(
        sq + count * jnp.square(total / count - mean) for total, sq in zip(sums, squares)
    ) / members
    rows = mean.shape[0]
    both_stats = exact_dot(
        jnp.concatenate([mean, lax.rsqrt(variance + EPS_NORM)], axis=0), pool, 3, NT
    )
    stat[0] = both_stats[0:rows]
    stat[1] = both_stats[rows:]

    def forward(b, carry):
        where = pl.ds(pl.multiple_of(b * area, area), area)
        x = feat[where, :].astype(F32)
        normed = (x - stat[0, pl.ds(b, 1), :]) * stat[1, pl.ds(b, 1), :]
        shifted = normed * gain[...] + bias[...]
        sig = jax.nn.sigmoid(shifted)
        nrm[where, :] = normed
        act[where, :] = (shifted * sig).astype(BF16)
        slope[where, :] = sig * (1.0 + shifted * (1.0 - sig))
        return carry

    lax.fori_loop(0, images, forward, 0)

    lane = lax.broadcasted_iota(jnp.int32, (8, cells), 1)
    col = lax.rem(lane, across)
    row = lax.rem(lane // across, height)

    def ahead(x, count):
        return pltpu.roll(x, (-count) % cells, 1) if count % cells else x

    def beside_col(x, off):
        if off == 0:
            return x
        ok = (col + off >= 0) & (col + off < across)
        return jnp.where(ok, ahead(x, off), 0.0)

    def above(x, arrived):
        edge = jnp.where(me > 0, ahead(arrived, (height - 1) * across), 0.0)
        return jnp.where(row == 0, edge, ahead(x, -across))

    def below(x, arrived):
        edge = jnp.where(me < n - 1, ahead(arrived, -(height - 1) * across), 0.0)
        return jnp.where(row == height - 1, edge, ahead(x, across))

    terms = dot(taps, act[...], NT)
    rows3 = []
    for dy in range(3):
        rows3.append(
            sum(
                beside_col(terms[(3 * dy + dx) * 8 : (3 * dy + dx + 1) * 8], dx - 1)
                for dx in range(3)
            )
        )
    halo[0] = rows3[0]
    halo[1] = rows3[2]
    halo_copies = [
        send(halo.at[0], halo_in.at[0], h_send.at[0], h_recv.at[0], following),
        send(halo.at[1], halo_in.at[1], h_send.at[1], h_recv.at[1], prev),
    ]
    over_x("b2")
    over_x("d")
    relay("x", "a", (("y", "a"), ("z", "a")))
    cell = lax.broadcasted_iota(jnp.int32, (cells, tokens), 0)
    tok = lax.broadcasted_iota(jnp.int32, (cells, tokens), 1)
    per_image = (height // PATCH) * tok_cols
    corner = (
        (tok // per_image) * area
        + (lax.rem(tok, per_image) // tok_cols) * (PATCH * across)
        + lax.rem(tok, tok_cols) * PATCH
    )
    away = cell - corner
    pick = [
        jnp.where(away == u * across + v, 1.0, 0.0).astype(BF16)
        for u in range(PATCH) for v in range(PATCH)
    ]
    arrive(v2)
    vfull[:, mine] = vhalf[...] + sum(v2_in[k].astype(F32) for k in range(ring))
    v3 = send(vfull.at[:, mine], vfull.at[:, mine], v_send.at[ring + 1], v_recv.at[ring + 1], sibling)
    arrive(halo_copies)
    relay("x", "b1", (("y", "b1"), ("z", "b1")))
    inner = PATCH * PATCH * LATENT
    latent = rows3[1] + above(rows3[0], halo_in[0]) + below(rows3[2], halo_in[1])
    first_half = lax.broadcasted_iota(jnp.int32, (8, tokens), 0) < LATENT
    blocks = []
    for u in range(PATCH):
        pair = [exact_dot(latent, pick[u * PATCH + v], 3) for v in range(PATCH)]
        blocks.append(jnp.where(first_half, pair[0], pair[1]))
    patches = jnp.concatenate(blocks, axis=0)
    p_hi, p_lo = split(patches, 2)
    pcat = jnp.concatenate([p_hi, p_lo, p_hi], axis=0).astype(BF16)
    v3.wait_recv()
    v_hi, v_lo = split(vfull[0:inner, :], 2)
    vcat[...] = jnp.concatenate([v_hi, v_hi, v_lo], axis=0).astype(BF16)
    pre_bias = vfull[inner : inner + 1, :] + winb[...]

    step = hidden // 4
    for c in range(4):
        where = slice(c * step, (c + 1) * step)
        pre = dot(pcat, vcat[:, where], TN) + pre_bias[:, where]
        sig = jax.nn.sigmoid(pre)
        hact[:, where] = (pre * sig).astype(BF16)
        hslope[:, where] = sig * (1.0 + pre * (1.0 - sig))
    relay("x", "b2", (("y", "b2"), ("z", "b2")))
    relay("y", "a", (("z", "e1"),))
    relay("z", "a", (("y", "e2"),))
    target = targ[...].astype(F32)
    unit_target = target * lax.rsqrt(jnp.sum(target * target, axis=1, keepdims=True) + EPS_UNIT)
    beside.wait_recv()
    pair_of = me // 2

    def pair_dot(j):
        base = lax.rem(pair_of + j, n // 2) * (2 * share)
        where = pl.ds(pl.multiple_of(base, 2 * share), 2 * share)
        return dot(hact[:, where], pout[where, :])

    bias_out = jnp.concatenate([woutb[i : i + 1, :] for i in range(woutb.shape[0])], axis=1)
    projected = pair_dot(0) + bias_out
    relay("y", "b1")
    relay("z", "b1")
    relay("x", "d")
    relay("y", "b2")
    relay("z", "b2")
    relay("z", "e1")
    relay("y", "e2")
    arrive(relays)
    for j in range(1, n // 2):
        projected = projected + pair_dot(j)
    inv_len = lax.rsqrt(jnp.sum(projected * projected, axis=1, keepdims=True) + EPS_UNIT)
    unit_proj = projected * inv_len
    cosine = jnp.sum(unit_proj * unit_target, axis=1, keepdims=True)
    grad_out = (-inv_len * (unit_target - cosine * unit_proj)).astype(BF16)
    for c in range(4):
        where = slice(c * step, (c + 1) * step)
        back = dot(grad_out, pout[where, :], NT)
        gh_ref[:, where] = (back * hslope[:, where]).astype(BF16)
    two = dot(vcat[inner:, :], gh_ref[...], NT)
    grad_patch = (two[0:inner] + two[inner:]).astype(BF16)

    grid = []
    for v in range(PATCH):
        grid.append(
            sum(
                dot(grad_patch[u * 8 : (u + 1) * 8], pick[u * PATCH + v], NT)
                for u in range(PATCH)
            )
        )
    low_rows = lax.broadcasted_iota(jnp.int32, (8, cells), 0) < LATENT
    both = jnp.where(low_rows, grid[0], grid[1])
    grad_lat = both + pltpu.roll(both, LATENT, 0)
    grad_lat = jnp.where(low_rows, grad_lat, 0.0)
    ghalo[...] = grad_lat
    ghalo_copies = [
        send(ghalo, ghalo_in.at[0], g_send.at[0], g_recv.at[0], following),
        send(ghalo, ghalo_in.at[1], g_send.at[1], g_recv.at[1], prev),
    ]
    wide = dot(pcat[0 : 2 * inner], gh_ref[...])
    a_sum = wide[0:inner] + wide[inner:]
    a_ref[...] = a_sum
    a16[...] = a_sum.astype(BF16)
    a_copies = spread(a16, a_in, a_send, a_recv)
    arrive(ghalo_copies)
    by_row = [below(grad_lat, ghalo_in[1]), grad_lat, above(grad_lat, ghalo_in[0])]
    grad_taps = jnp.concatenate(
        [beside_col(by_row[dy], 1 - dx) for dy in range(3) for dx in range(3)], axis=0
    ).astype(BF16)
    gs_ref[...] = dot(grad_taps, taps, TN)
    conv = dot(grad_taps, act[...])

    def backward(b, carry):
        where = pl.ds(pl.multiple_of(b * area, area), area)
        gs = gs_ref[where, :] * slope[where, :]
        gs_ref[where, :] = gs
        fs[0, pl.ds(b, 1), :] = jnp.sum(gs, axis=0, keepdims=True)
        fs[1, pl.ds(b, 1), :] = jnp.sum(gs * nrm[where, :], axis=0, keepdims=True)
        return carry

    lax.fori_loop(0, images, backward, 0)
    pooled = exact_dot(jnp.concatenate([fs[0] * gain[...], fs[1] * gain[...]], axis=0), pool, 3)
    fg[0] = pooled[0:rows]
    fg[1] = pooled[rows:]
    f_copies = spread(fg, fg_in, f_send, f_recv)
    gain_row = jnp.sum(fs[1], axis=0, keepdims=True)
    bias_row = jnp.sum(fs[0], axis=0, keepdims=True)
    row8 = lax.broadcasted_iota(jnp.int32, (8, channels), 0)
    per = pack.shape[1] // 8
    lanes = pack.shape[2]
    for i in range(5):
        part_i = conv[16 * i : 16 * i + 8]
        if i < 4:
            part_i = part_i + pltpu.roll(conv[16 * i + 8 : 16 * i + 16], LATENT, 0)
        else:
            part_i = jnp.where(row8 == LATENT, gain_row, part_i)
            part_i = jnp.where(row8 == LATENT + 1, bias_row, part_i)
        for c in range(channels // lanes):
            t = 5 * c + i
            pack[t // per, (t % per) * 8 : (t % per + 1) * 8, :] = (
                part_i[:, c * lanes : (c + 1) * lanes]
            )
    for t in range(5 * (channels // lanes), n * per):
        pack[t // per, (t % per) * 8 : (t % per + 1) * 8, :] = jnp.zeros((8, lanes), F32)
    p_copies = []
    for k in range(1, n):
        peer = lax.rem(me + k, n)
        p_copies.append(
            send(pack.at[peer], pack_in.at[k - 1], p_send.at[k - 1], p_recv.at[k - 1], peer)
        )
    arrive(a_copies)
    a_all = a_ref[...] + sum(a_in[k].astype(F32) for k in range(n - 1))
    emb[...] = exact_dot(a_all, win[...], 2, NT).astype(BF16)
    q_copies = across_batch(emb, emb_in, e_send, e_recv)
    arrive(p_copies)
    piece[...] = (pack[me] + sum(pack_in[k] for k in range(n - 1))).astype(BF16)
    piece_copies = across_batch(piece, piece_in, q_send, q_recv)
    arrive(f_copies)
    totals = [(fg[i] + sum(fg_in[k, i] for k in range(n - 1))) / members for i in range(2)]
    both_means = exact_dot(jnp.concatenate(totals, axis=0), pool, 3, NT)
    stat[2] = both_means[0:rows]
    stat[3] = both_means[rows:]

    def finish(b, carry):
        where = pl.ds(pl.multiple_of(b * area, area), area)
        one = pl.ds(b, 1)
        out[where, :] = (
            stat[1, one, :]
            * (gs_ref[where, :] * gain[...] - stat[2, one, :] - nrm[where, :] * stat[3, one, :])
        ).astype(BF16)
        return carry

    lax.fori_loop(0, images, finish, 0)
    arrive(q_copies)
    whole_emb[me] = ordered(emb, emb_in, group, nb)
    w_copies = []
    for k in range(1, n):
        peer = lax.rem(me + k, n)
        w_copies.append(
            send(whole_emb.at[me], whole_emb.at[me], y_send.at[k - 1], y_recv.at[k - 1], peer)
        )
    arrive(piece_copies)
    whole[me] = ordered(piece, piece_in, group, nb)
    for k in range(1, n):
        peer = lax.rem(me + k, n)
        w_copies.append(send(whole.at[me], whole.at[me], w_send.at[k - 1], w_recv.at[k - 1], peer))
    arrive(w_copies)
    for c in range(channels // lanes):
        at = slice(c * lanes, (c + 1) * lanes)
        for i in range(5):
            t = 5 * c + i
            tile = whole[t // per, (t % per) * 8 : (t % per + 1) * 8, :]
            for side in range(2):
                tap = 2 * i + side
                tile_rows = tile[side * LATENT : (side + 1) * LATENT]
                if tap < 9:
                    start = tap * channels + c * lanes
                    conv_o[:, start : start + lanes] = tile_rows
                else:
                    gain_o[:, at] = tile_rows[0:1]
                    bias_o[:, at] = tile_rows[1:2]
    for k in range(n):
        emb_o[:, k * part : (k + 1) * part] = whole_emb[k]
    for copy in sent:
        copy.wait_send()


def ordered(own, arrived, group, nb):
    total = None
    for g in range(nb):
        slot = lax.rem(group + nb - g, nb)
        value = arrived[jnp.maximum(slot - 1, 0)] if nb > 1 else own[...]
        value = jnp.where(slot == 0, own[...].astype(F32), value.astype(F32))
        total = value if total is None else total + value
    return total


def store(*refs):
    count = (len(refs) - 1) // 2
    sem = refs[-1]
    copies = [
        pltpu.make_async_copy(refs[i], refs[count + i], sem.at[i]) for i in range(count)
    ]
    for copy in copies:
        copy.start()
    for copy in copies:
        copy.wait()


def shards(
    features, norm_gain, norm_bias, conv_weight, embed_weight, embed_bias,
    proj_in, proj_in_bias, proj_out, proj_out_bias, targets,
):
    images, height, across, channels = features.shape
    n = lax.axis_size("rows")
    nb = lax.axis_size("batch")
    lanes = 128
    per = -(-(5 * (channels // lanes)) // n)
    cells = images * height * across
    align = targets.shape[-1]
    tokens = targets.shape[0] * targets.shape[1] * targets.shape[2]
    inner, width = embed_weight.shape
    part, hidden = proj_in.shape
    share = proj_out.shape[0]
    pad_images = -(-images // 8) * 8
    sliced = part % lanes == 0
    embed_bias = embed_bias[None]
    if not sliced:
        me = lax.axis_index("rows")
        embed_weight = lax.dynamic_slice_in_dim(embed_weight, me * part, part, axis=1)
        embed_bias = lax.dynamic_slice_in_dim(embed_bias, me * part, part, axis=1)
    ring = n // 2 - 1
    cols = hidden // 2
    last = max(nb - 1, 1)
    reserve = 2 * cells * channels + 4 * (8 * 9 * channels + 16 * channels + inner * width)
    dma = pltpu.SemaphoreType.DMA
    vm = pltpu.VMEM
    results = pl.pallas_call(
        functools.partial(kernel, images, height, across, n, nb, sliced),
        out_shape=(
            vm((cells, channels), BF16),
            vm((LATENT, 9 * channels), F32),
            vm((1, channels), F32),
            vm((1, channels), F32),
            vm((inner, width), F32),
        ),
        in_specs=[pl.BlockSpec(memory_space=pltpu.HBM)] * 11,
        out_specs=[pl.BlockSpec(memory_space=vm)] * 5,
        scratch_shapes=[
            vm((cells, channels), BF16),
            vm((1, channels), F32),
            vm((1, channels), F32),
            vm((LATENT, 9 * channels), BF16),
            vm((inner, part), F32),
            vm((1, part), F32),
            vm((part, hidden), BF16),
            vm((1, hidden), F32),
            vm((align // lanes, lanes), F32),
            vm((tokens, align), BF16),
            vm((2, pad_images, channels), F32),
            vm((2, pad_images, lanes), F32),
            vm((n - 1, 2, pad_images, lanes), F32),
            vm((cells, channels), F32),
            vm((cells, channels), F32),
            vm((cells, channels), BF16),
            vm((cells, channels), F32),
            vm((2, 8, cells), F32),
            vm((2, 8, cells), F32),
            vm((8, cells), F32),
            vm((2, 8, cells), F32),
            vm((inner + 8, hidden), F32),
            vm((inner + 8, cols), F32),
            vm((inner + 8, cols), F32),
            vm((inner + 8, cols), BF16),
            vm((max(ring, 1), inner + 8, cols), BF16),
            vm((inner + 8, hidden), F32),
            vm((3 * inner, hidden), BF16),
            vm((n * share, align), BF16),
            vm((tokens, hidden), BF16),
            vm((tokens, hidden), F32),
            vm((tokens, hidden), BF16),
            vm((inner, hidden), F32),
            vm((inner, hidden), BF16),
            vm((n - 1, inner, hidden), BF16),
            vm((2, pad_images, channels), F32),
            vm((2, pad_images, lanes), F32),
            vm((n - 1, 2, pad_images, lanes), F32),
            vm((4, pad_images, channels), F32),
            vm((n, per * 8, lanes), F32),
            vm((n - 1, per * 8, lanes), F32),
            vm((per * 8, lanes), BF16),
            vm((last, per * 8, lanes), BF16),
            vm((inner, part), BF16),
            vm((last, inner, part), BF16),
            vm((n, per * 8, lanes), F32),
            vm((n, inner, part), F32),
            dma((11,)), dma((n - 1,)), dma((n - 1,)),
            dma((ring + 2,)), dma((ring + 2,)),
            dma((24 * ring + 1,)), dma((24 * ring + 1,)),
            dma((2,)), dma((2,)), dma((2,)), dma((2,)),
            dma((n - 1,)), dma((n - 1,)), dma((n - 1,)), dma((n - 1,)),
            dma((n - 1,)), dma((n - 1,)),
            dma((last,)), dma((last,)), dma((last,)), dma((last,)),
            dma((n - 1,)), dma((n - 1,)), dma((n - 1,)), dma((n - 1,)),
        ],
        compiler_params=pltpu.CompilerParams(
            collective_id=0, has_side_effects=True, vmem_limit_bytes=67043328 - reserve
        ),
        name="alignment_step",
    )(
        features.reshape(cells, channels), norm_gain[None], norm_bias[None], conv_weight,
        embed_weight, embed_bias, proj_in, proj_in_bias[None], proj_out,
        proj_out_bias.reshape(align // lanes, lanes), targets.reshape(tokens, align),
    )
    grad_features, grad_conv, grad_gain, grad_bias, grad_embed = pl.pallas_call(
        store,
        out_shape=tuple(jax.ShapeDtypeStruct(x.shape, x.dtype) for x in results),
        in_specs=[pl.BlockSpec(memory_space=vm)] * 5,
        out_specs=[pl.BlockSpec(memory_space=pltpu.HBM)] * 5,
        scratch_shapes=[dma((5,))],
        compiler_params=pltpu.CompilerParams(vmem_limit_bytes=4 * 1024 * 1024),
        name="store_results",
    )(*results)
    return (
        grad_features.reshape(images, height, across, channels),
        grad_conv, grad_gain[0], grad_bias[0], grad_embed,
    )


def solution(mesh):
    in_specs = (
        P("batch", "rows", None, None), P(), P(), P(), P(), P(),
        P("rows", None), P(), P("rows", None), P(), P("batch", "rows", None, None),
    )
    out_specs = (P("batch", "rows", None, None), P(), P(), P(), P())
    return jax.shard_map(shards, mesh=mesh, in_specs=in_specs, out_specs=out_specs, check_vma=False)
```
